32 devices in a mesh: dp: 4 (over y, z), sp: 8 (over x, core).
Axes of the slice: x: 4, y: 2, z: 2, core: 2. Of those that a mesh axis runs over, the one named last changes fastest.
The devices are a block of a 4x4x8 slice.
Arguments:
- x_patch: bfloat16 [64, 4096, 1024], P('dp', 'sp'), parts along dimension 0
- w_tok1: bfloat16 [4096, 512], P('sp')
- b_tok1: float32 [512], P('sp')
- w_tok2: bfloat16 [512, 4096], P(None, 'sp')
- b_tok2: float32 [4096], P('sp')
- w_ch1: bfloat16 [1024, 4096], replicated
- b_ch1: float32 [4096], replicated
- w_ch2: bfloat16 [4096, 1024], replicated
- b_ch2: float32 [1024], replicated
- ln1_gain: float32 [1024], replicated
- ln1_bias: float32 [1024], replicated
- ln2_gain: float32 [1024], replicated
- ln2_bias: float32 [1024], replicated
Outputs:
- output: bfloat16 [64, 4096, 1024], P('dp', 'sp'), parts along dimension 0
There are 4 independent parts. The reference program is written for one: setup_inputs(seed, part) draws one part's arguments, and reference() takes and returns one part's arrays. A program takes and returns all parts, laid end to end along the dimension named above; an argument that names none is the same for every part.
All inputs are finite; a program needn't handle non-finite values.
Results may differ from the reference program's by a relative error of at most 0.00987663.
Values are sent between devices in bfloat16 or wider.
A program may use at most 768 MiB of HBM per device.

```python
import jax
import jax.numpy as jnp
from jax import lax

BATCH = 16
PATCHES = 4096
CHANNELS = 1024
TOKEN_HID = 512
CHAN_HID = 4096
LN_EPS = 1e-6


def draw_normal(rng_key, out_shape, spread):
    return jax.random.normal(rng_key, out_shape, jnp.float32) * spread


def setup_inputs(seed: int = 0, part: int = 0) -> dict:
    shared = jax.random.split(jax.random.key(seed), 12)
    x_key = jax.random.fold_in(jax.random.key(seed + 1), part)
    x_patch = jax.random.normal(x_key, (BATCH, PATCHES, CHANNELS), jnp.float32)
    return {
        "x_patch": x_patch.astype(jnp.bfloat16),
        "w_tok1": draw_normal(shared[0], (PATCHES, TOKEN_HID), PATCHES ** -0.5).astype(jnp.bfloat16),
        "b_tok1": draw_normal(shared[1], (TOKEN_HID,), 0.5),
        "w_tok2": draw_normal(shared[2], (TOKEN_HID, PATCHES), TOKEN_HID ** -0.5).astype(jnp.bfloat16),
        "b_tok2": draw_normal(shared[3], (PATCHES,), 0.5),
        "w_ch1": draw_normal(shared[4], (CHANNELS, CHAN_HID), CHANNELS ** -0.5).astype(jnp.bfloat16),
        "b_ch1": draw_normal(shared[5], (CHAN_HID,), 0.5),
        "w_ch2": draw_normal(shared[6], (CHAN_HID, CHANNELS), CHAN_HID ** -0.5).astype(jnp.bfloat16),
        "b_ch2": draw_normal(shared[7], (CHANNELS,), 0.3),
        "ln1_gain": 1.0 + draw_normal(shared[8], (CHANNELS,), 0.2),
        "ln1_bias": draw_normal(shared[9], (CHANNELS,), 0.3),
        "ln2_gain": 1.0 + draw_normal(shared[10], (CHANNELS,), 0.2),
        "ln2_bias": draw_normal(shared[11], (CHANNELS,), 0.3),
    }


def layer_norm(values, ln_gain, ln_bias):
    mean_val = jnp.mean(values, axis=-1, keepdims=True)
    centred = values - mean_val
    var_val = jnp.mean(centred * centred, axis=-1, keepdims=True)
    return centred * lax.rsqrt(var_val + LN_EPS) * ln_gain + ln_bias


def reference(x_patch, w_tok1, b_tok1, w_tok2, b_tok2, w_ch1, b_ch1, w_ch2, b_ch2, ln1_gain, ln1_bias, ln2_gain, ln2_bias):
    def one_image(x_img):
        x_wide = x_img.astype(jnp.float32)
        normed = layer_norm(x_wide, ln1_gain, ln1_bias).astype(jnp.bfloat16)
        tok_pre = jnp.dot(w_tok1.T, normed, preferred_element_type=jnp.float32) + b_tok1[:, None]
        tok_act = jax.nn.gelu(tok_pre).astype(jnp.bfloat16)
        tok_out = jnp.dot(w_tok2.T, tok_act, preferred_element_type=jnp.float32) + b_tok2[:, None]
        x_mid = (x_wide + tok_out).astype(jnp.bfloat16)
        mid_wide = x_mid.astype(jnp.float32)
        normed_two = layer_norm(mid_wide, ln2_gain, ln2_bias).astype(jnp.bfloat16)
        ch_pre = jnp.dot(normed_two, w_ch1, preferred_element_type=jnp.float32) + b_ch1
        ch_act = jax.nn.gelu(ch_pre).astype(jnp.bfloat16)
        ch_out = jnp.dot(ch_act, w_ch2, preferred_element_type=jnp.float32) + b_ch2
        return (mid_wide + ch_out).astype(jnp.bfloat16)

    return lax.map(one_image, x_patch)
```

```python
import functools

import jax
import jax.numpy as jnp
from jax import lax
from jax.experimental import pallas as pl
from jax.experimental.pallas import tpu as pltpu
from jax.sharding import PartitionSpec as P

LN_EPS = 1e-6
MESH = pl.DeviceIdType.MESH
F32 = jnp.float32
BF16 = jnp.bfloat16
LAG = 6
XS = LAG + 3
GS = LAG
CW = 512
LB = 64
TANH_A = 0.7978845608028654
TANH_B = 0.7978845608028654 * 0.044715


def gelu(a):
    half = 0.5 * a
    return half + half * jnp.tanh(a * (TANH_A + TANH_B * (a * a)))


def norm(values, gain, bias):
    mean = jnp.mean(values, axis=-1, keepdims=True)
    centred = values - mean
    var = jnp.mean(centred * centred, axis=-1, keepdims=True)
    return centred * lax.rsqrt(var + LN_EPS) * gain + bias


def dot(a, b):
    return jnp.dot(a, b, preferred_element_type=F32)


def layer_kernel(n, x_hbm, w1_hbm, w2_hbm, wc1_hbm, wc2_hbm, b1_ref, b2_ref, bc1_ref, bc2_ref, g1_ref, o1_ref, g2_ref, o2_ref,
                 z_hbm, w1, w2, wc1, wc2, xs, us, part, sums, pair_in, hop1_out, hop1_in, hop2_out, hop2_in, gs,
                 x1s, vs, act0, act1, acc, zs,
                 w_sem, x_sem, z_sem, p_send, p_recv, h1_send, h1_recv, h2_send, h2_recv, a1_send, a1_recv, a2_send, a2_recv,
                 a3_send, a3_recv):
    images, rows, chans = x_hbm.shape
    own = b1_ref.shape[0]
    half_c = chans // 2
    wide = wc1.shape[1]
    chips = n // 2
    me = lax.axis_index("sp")
    core = lax.rem(me, 2)
    chip = me // 2
    chip_r = lax.rem(chip + 1, chips)
    chip_l = lax.rem(chip + chips - 1, chips)
    chip_o = lax.rem(chip + 2, chips)
    right = 2 * chip_r + core
    left = 2 * chip_l + core
    pair = 2 * chip + 1 - core
    opposite = 2 * chip_o + core

    def remote(src, dst, send, recv, to):
        return pltpu.make_async_remote_copy(src_ref=src, dst_ref=dst, send_sem=send, recv_sem=recv,
                                            device_id={"sp": to}, device_id_type=MESH)

    def x_copy(i):
        slot = lax.rem(i, XS)
        return pltpu.make_async_copy(x_hbm.at[i], xs.at[slot], x_sem.at[slot])

    def z_copy(i):
        slot = lax.rem(i, 2)
        return pltpu.make_async_copy(zs.at[slot], z_hbm.at[i], z_sem.at[slot])

    def w_copy(k, src, dst):
        return pltpu.make_async_copy(src, dst, w_sem.at[k])

    def chunk(q):
        return pl.ds(pl.multiple_of(q * own, own), own)

    def g_rows(slot, dev):
        return gs.at[slot, pl.ds(pl.multiple_of(dev * own, own), own), :]

    def pair_copy(i):
        slot = lax.rem(i, 2)
        return remote(part, pair_in.at[slot], p_send, p_recv.at[slot], pair)

    def hop1_copy(i, d):
        slot = lax.rem(i, 2)
        return remote(hop1_out.at[d], hop1_in.at[slot, d], h1_send.at[d], h1_recv.at[slot, d], (right, left)[d])

    def hop2_copy(i, d):
        slot = lax.rem(i, 2)
        return remote(hop2_out.at[d], hop2_in.at[slot, d], h2_send.at[d], h2_recv.at[slot, d], (right, left)[d])

    def gather1_copy(i, d):
        slot, par = lax.rem(i, GS), lax.rem(i, 2)
        mine = g_rows(slot, me)
        return remote(mine, mine, a1_send.at[d], a1_recv.at[par, d], (right, left, pair)[d])

    def gather2_copy(i, d):
        slot, par = lax.rem(i, GS), lax.rem(i, 2)
        source = (left, right, left, right)[d]
        if d < 2:
            block = gs.at[slot, pl.ds(pl.multiple_of(source * own, own), own), pl.ds(d * half_c, half_c)]
        else:
            block = g_rows(slot, source)
        return remote(block, block, a2_send.at[d], a2_recv.at[par, d], (right, left, pair, pair)[d])

    def gather3_copy(i):
        slot, par = lax.rem(i, GS), lax.rem(i, 2)
        block = g_rows(slot, opposite)
        return remote(block, block, a3_send, a3_recv.at[par], pair)

    def stage0(i):
        xslot, slot = lax.rem(i, XS), lax.rem(i, 3)
        for r in range(0, rows, LB):
            us[r:r + LB, :] = norm(xs[xslot, r:r + LB, :].astype(F32), g1_ref[...], o1_ref[...]).astype(BF16)
        side = part.shape[0]
        theirs = pl.ds(pl.multiple_of((1 - core) * side, side), side)
        mine = pl.ds(pl.multiple_of(core * side, side), side)
        for c in range(0, chans, 256):
            u = us[:, c:c + 256]
            part[:, c:c + 256] = dot(w1[theirs, :], u)
            sums[slot, :, c:c + 256] = dot(w1[mine, :], u)

    def stage1(i):
        slot, par = lax.rem(i, 3), lax.rem(i, 2)
        pair_copy(i).wait()
        for q in range(chips):
            r = slice(q * own, (q + 1) * own)
            sums[slot, r, :] = sums[slot, r, :] + pair_in[par, r, :]
        far = sums[slot, chunk(chip_o), :]
        hop1_out[0] = far[:, :half_c].astype(BF16)
        hop1_out[1] = far[:, half_c:].astype(BF16)

    def stage2(i):
        slot, par = lax.rem(i, 3), lax.rem(i, 2)
        for d in range(2):
            hop1_copy(i, d).wait()
        to_right = sums[slot, chunk(chip_r), :]
        hop2_out[0, :, :half_c] = (to_right[:, :half_c] + hop1_in[par, 0].astype(F32)).astype(BF16)
        hop2_out[0, :, half_c:] = to_right[:, half_c:].astype(BF16)
        to_left = sums[slot, chunk(chip_l), :]
        hop2_out[1, :, :half_c] = to_left[:, :half_c].astype(BF16)
        hop2_out[1, :, half_c:] = (to_left[:, half_c:] + hop1_in[par, 1].astype(F32)).astype(BF16)

    def stage3(i):
        slot, par = lax.rem(i, 3), lax.rem(i, 2)
        for d in range(2):
            hop2_copy(i, d).wait()
        h = sums[slot, chunk(chip), :] + hop2_in[par, 0].astype(F32) + hop2_in[par, 1].astype(F32) + b1_ref[...]
        gs[lax.rem(i, GS), chunk(me), :] = gelu(h).astype(BF16)

    def send1(i):
        for d in range(2):
            hop1_copy(i, d).start()

    def send2(i):
        for d in range(2):
            hop2_copy(i, d).start()

    def send3(i):
        for d in range(3):
            gather1_copy(i, d).start()

    def got(sem, region):
        pltpu.make_async_copy(region, region, sem).wait()

    def stage4(i):
        slot, par = lax.rem(i, GS), lax.rem(i, 2)
        for d in range(3):
            gather1_copy(i, d).wait_send()
            got(a1_recv.at[par, d], g_rows(slot, (left, right, pair)[d]))
        for d in range(4):
            gather2_copy(i, d).start()

    def stage5(i):
        slot, par = lax.rem(i, GS), lax.rem(i, 2)
        far = pl.ds(pl.multiple_of(opposite * own, own), own)
        for d in range(4):
            gather2_copy(i, d).wait_send()
        for d in range(2):
            got(a2_recv.at[par, d], gs.at[slot, far, pl.ds(d * half_c, half_c)])
        for d in range(2):
            got(a2_recv.at[par, 2 + d], g_rows(slot, 2 * (chip_l, chip_r)[d] + 1 - core))
        gather3_copy(i).start()

    def stage6_ready(i):
        slot, par = lax.rem(i, GS), lax.rem(i, 2)
        gather3_copy(i).wait_send()
        got(a3_recv.at[par], g_rows(slot, 2 * chip_o + 1 - core))

    def stage6(i):
        xslot, slot, zslot = lax.rem(i, XS), lax.rem(i, GS), lax.rem(i, 2)
        for r in range(0, rows, 256):
            for c in range(0, chans, 256):
                t = dot(w2[r:r + 256, :], gs[slot, :, c:c + 256]) + b2_ref[r:r + 256, :]
                x1s[r:r + 256, c:c + 256] = (xs[xslot, r:r + 256, c:c + 256].astype(F32) + t).astype(BF16)
            for q in range(r, r + 256, LB):
                vs[q:q + LB, :] = norm(x1s[q:q + LB, :].astype(F32), g2_ref[...], o2_ref[...]).astype(BF16)
        acts = (act0, act1)
        steps = wide // CW

        def up(k):
            for c in range(0, CW, 256):
                col = slice(k * CW + c, k * CW + c + 256)
                pre = dot(vs[...], wc1[:, col]) + bc1_ref[:, col]
                acts[k % 2][:, c:c + 256] = gelu(pre).astype(BF16)

        def down(k):
            for c in range(0, chans, 256):
                piece = dot(acts[k % 2][...], wc2[k * CW:(k + 1) * CW, c:c + 256])
                if k == 0:
                    acc[:, c:c + 256] = piece
                elif k < steps - 1:
                    acc[:, c:c + 256] = acc[:, c:c + 256] + piece
                else:
                    total = acc[:, c:c + 256] + piece + bc2_ref[:, c:c + 256]
                    zs[zslot, :, c:c + 256] = (x1s[:, c:c + 256].astype(F32) + total).astype(BF16)

        up(0)
        for k in range(1, steps):
            up(k)
            down(k - 1)
        down(steps - 1)

    def comm(t, guard):
        for k, stage in ((5, stage5), (4, stage4), (3, stage3), (2, stage2), (1, stage1)):
            guard(t - k, stage)
        for k, send in ((3, send3), (2, send2), (1, send1)):
            guard(t - k, send)

    def always(i, stage):
        stage(i)

    def guarded(i, stage):
        @pl.when(jnp.logical_and(i >= 0, i < images))
        def _():
            stage(i)

    x_copy(0).start()
    w_copy(0, w1_hbm, w1).start()
    barrier = pltpu.get_barrier_semaphore()
    for dev in (left, right, pair):
        pl.semaphore_signal(barrier, inc=1, device_id={"sp": dev}, device_id_type=MESH)
    pl.semaphore_wait(barrier, 3)
    x_copy(1).start()
    w_copy(0, w1_hbm, w1).wait()
    w_copy(1, w2_hbm, w2).start()
    w_copy(2, wc1_hbm, wc1).start()
    w_copy(3, wc2_hbm, wc2).start()

    @pl.loop(0, LAG)
    def _(t):
        comm(t, guarded)
        x_copy(t).wait()
        x_copy(t + 2).start()
        stage0(t)
        pair_copy(t).start()

    w_copy(1, w2_hbm, w2).wait()
    w_copy(2, wc1_hbm, wc1).wait()
    w_copy(3, wc2_hbm, wc2).wait()

    def z_free(i):
        @pl.when(i >= 2)
        def _():
            z_copy(i - 2).wait()

    @pl.loop(LAG, images)
    def _(t):
        stage6_ready(t - LAG)
        comm(t, always)
        x_copy(t).wait()

        @pl.when(t + 2 < images)
        def _():
            x_copy(t + 2).start()

        z_free(t - LAG)
        stage0(t)
        pair_copy(t).start()
        stage6(t - LAG)
        z_copy(t - LAG).start()

    @pl.loop(images, images + LAG)
    def _(t):
        stage6_ready(t - LAG)
        comm(t, guarded)
        z_free(t - LAG)
        stage6(t - LAG)
        z_copy(t - LAG).start()

    z_copy(images - 2).wait()
    z_copy(images - 1).wait()


def solution(mesh):
    n = mesh.shape["sp"]
    row_spec = P("dp", "sp", None)

    def local_layer(x, w1, b1, w2, b2, wc1, bc1, wc2, bc2, g1, o1, g2, o2):
        images, rows, chans = x.shape
        hid = w1.shape[1]
        own = b1.shape[0]
        wide = wc1.shape[1]
        chips = n // 2
        w1t = w1.T.reshape(chips, 2, own, rows).transpose(1, 0, 2, 3).reshape(hid, rows)
        vmem = pl.BlockSpec(memory_space=pltpu.VMEM)
        hbm = pl.BlockSpec(memory_space=pl.ANY)
        dma = pltpu.SemaphoreType.DMA
        return pl.pallas_call(
            functools.partial(layer_kernel, n),
            name="mixer_layer",
            out_shape=jax.ShapeDtypeStruct(x.shape, BF16),
            in_specs=[hbm] * 5 + [vmem] * 8,
            out_specs=hbm,
            scratch_shapes=[
                pltpu.VMEM((hid, rows), BF16),
                pltpu.VMEM((rows, hid), BF16),
                pltpu.VMEM((chans, wide), BF16),
                pltpu.VMEM((wide, chans), BF16),
                pltpu.VMEM((XS, rows, chans), BF16),
                pltpu.VMEM((rows, chans), BF16),
                pltpu.VMEM((hid // 2, chans), F32),
                pltpu.VMEM((3, hid // 2, chans), F32),
                pltpu.VMEM((2, hid // 2, chans), F32),
                pltpu.VMEM((2, own, chans // 2), BF16),
                pltpu.VMEM((2, 2, own, chans // 2), BF16),
                pltpu.VMEM((2, own, chans), BF16),
                pltpu.VMEM((2, 2, own, chans), BF16),
                pltpu.VMEM((GS, hid, chans), BF16),
                pltpu.VMEM((rows, chans), BF16),
                pltpu.VMEM((rows, chans), BF16),
                pltpu.VMEM((rows, CW), BF16),
                pltpu.VMEM((rows, CW), BF16),
                pltpu.VMEM((rows, chans), F32),
                pltpu.VMEM((2, rows, chans), BF16),
                dma((4,)), dma((XS,)), dma((2,)),
                dma, dma((2,)),
                dma((2,)), dma((2, 2)),
                dma((2,)), dma((2, 2)),
                dma((3,)), dma((2, 3)),
                dma((4,)), dma((2, 4)),
                dma, dma((2,)),
            ],
            compiler_params=pltpu.CompilerParams(collective_id=0, has_side_effects=True, vmem_limit_bytes=66_000_000),
        )(x, w1t, w2.T, wc1, wc2, b1[:, None], b2[:, None], bc1[None, :], bc2[None, :], g1[None, :], o1[None, :], g2[None, :], o2[None, :])

    in_specs = (row_spec, P("sp", None), P("sp"), P(None, "sp"), P("sp"), P(None, None), P(None), P(None, None), P(None),
                P(None), P(None), P(None), P(None))
    return jax.shard_map(local_layer, mesh=mesh, in_specs=in_specs, out_specs=row_spec, check_vma=False)
```
